32 devices in a mesh: occ: 2 (over x), vir: 4 (over z), aux: 4 (over y, core).
Axes of the slice: x: 2, y: 2, z: 4, core: 2. Of those that a mesh axis runs over, the one named last changes fastest.
Arguments:
- amplitudes: bfloat16 [16, 1024, 1024], P('occ', 'vir'), may hold values from -6 to 6
- pair_mask: int32 [16, 8, 8], P('occ', 'vir'), may hold values 0 or 1
- left_factor: bfloat16 [32, 1024, 4096], P(None, 'vir', 'aux'), may hold values from -0.0390625 to 0.0390625
- left_mask: int32 [8, 32], P('vir', 'aux'), may hold values 0 or 1
- right_factor: bfloat16 [1024, 4, 4096], P(('occ', 'vir'), None, 'aux'), may hold values from -0.0390625 to 0.0390625
- right_mask: int32 [8, 32], P(None, 'aux'), may hold values 0 or 1
- residual_in: float32 [16, 4, 32], P('occ'), may hold values from -6 to 6
Outputs:
- updated: float32 [16, 4, 32], P('occ')
The draws below stay inside these ranges and needn't reach their ends.
All inputs are finite; a program needn't handle non-finite values. No bound on the sum of `pair_mask` or of `left_mask` or of `right_mask` on one device may be relied on, other than what follows from the above.
Results may differ from the reference program's by a relative error of at most 0.0003.
Values may be sent and summed in bfloat16 or wider, within the bound.
A program may use at most 128 MiB of HBM per device.

```python
import jax
import jax.numpy as jnp
from jax import lax

V = 1024
NAUX = 4096
TILE = 128
AW = 32
BW = 4
PAIRS = 16
NVT = 8
NQT = 32


def set_ends(entries, own_key, smallest, top_value):
    dims = entries.shape
    place = [jax.random.randint(jax.random.fold_in(own_key, axis), (), 0, dims[axis]) for axis in range(len(dims))]
    entries = entries.at[tuple(place)].set(smallest)
    longest = dims.index(max(dims))
    place[longest] = (place[longest] + 1) % dims[longest]
    return entries.at[tuple(place)].set(top_value)


def block_levels(rng, dims, cuts, low, high):
    def one(dim, parts):
        draws = jax.random.uniform(jax.random.fold_in(jax.random.fold_in(rng, 6), dim), (parts,), jnp.float32, low / len(cuts), high / len(cuts))
        return jnp.repeat(jnp.exp(draws), dims[dim] // parts).reshape((-1,) + (1,) * (len(dims) - dim - 1))

    level = one(*cuts[0])
    for cut in cuts[1:]:
        level = level * one(*cut)
    return level


def scatter_about(rng, shape, spread, bound, split=(), kind=jnp.bfloat16):
    drawn = spread * jax.random.normal(rng, shape, jnp.float32)
    if split:
        drawn = drawn * block_levels(rng, shape, split, -0.22, 0.18)
    return jnp.clip(drawn, -bound, bound).astype(kind)


def setup_inputs(seed: int = 0) -> dict:
    key_list = jax.random.split(jax.random.key(seed), 8)
    return {
        "amplitudes": scatter_about(key_list[0], (PAIRS, V, V), 1.0, 6.0, ((0, 2), (1, 4))),
        "pair_mask": set_ends((jax.random.randint(key_list[1], (PAIRS, NVT, NVT), 0, 4) < 3).astype(jnp.int32), jax.random.fold_in(key_list[1], 1), 0, 1),
        "left_factor": scatter_about(key_list[2], (AW, V, NAUX), (V * max(2, NAUX // 150)) ** -0.5, 0.0390625, ((1, 4), (2, 4))),
        "left_mask": set_ends((jax.random.randint(key_list[3], (NVT, NQT), 0, 2) < 1).astype(jnp.int32), jax.random.fold_in(key_list[3], 1), 0, 1),
        "right_factor": scatter_about(key_list[4], (V, BW, NAUX), (V * max(2, NAUX // 150)) ** -0.5, 0.0390625, ((0, 8), (2, 4))),
        "right_mask": set_ends((jax.random.randint(key_list[5], (NVT, NQT), 0, 2) < 1).astype(jnp.int32), jax.random.fold_in(key_list[5], 1), 0, 1),
        "residual_in": scatter_about(key_list[6], (PAIRS, BW, AW), 1.0, 6.0, ((0, 2),), jnp.float32),
    }


def expand_tiles(mask, width):
    grown = jnp.repeat(jnp.repeat(mask, width, axis=-2), width, axis=-1)
    return grown.astype(jnp.float32)


def reference(amplitudes, pair_mask, left_factor, left_mask, right_factor, right_mask, residual_in):
    left = left_factor.astype(jnp.float32) * expand_tiles(left_mask, TILE)[None, :, :]
    right = right_factor.astype(jnp.float32) * expand_tiles(right_mask, TILE)[:, None, :]
    right_flat = right.reshape(V, BW * NAUX)

    def one_pair(pieces):
        amp, msk = pieces
        tau = amp.astype(jnp.float32) * expand_tiles(msk, TILE)
        inner = jnp.dot(tau, right_flat, precision=lax.Precision.HIGHEST, preferred_element_type=jnp.float32)
        inner = inner.reshape(V, BW, NAUX)
        return jnp.einsum("cbq,acq->ba", inner, left, precision=lax.Precision.HIGHEST)

    ladder = lax.map(one_pair, (amplitudes, pair_mask))
    return residual_in + ladder
```

```python
import functools

import jax
import jax.numpy as jnp
from jax import lax
from jax.experimental import pallas as pl
from jax.experimental.pallas import tpu as pltpu
from jax.sharding import PartitionSpec as P

TILE = 128
QC = 128
CC = 32
AHEAD = 4
MESH = pl.DeviceIdType.MESH
F32 = jnp.float32
BF16 = jnp.bfloat16


def kernel(
    no, nv, na, pair_mask, left_mask, right_mask, amp_hbm, left_hbm, right_hbm, res,
    out, raw, amp, left, rbuf, tau, tsend, lhs_a, rhs_a, lhs_b, rhs_b, acc, part, parts,
    amp_sem, left_sem, raw_sem, r_send, r_recv, t_send, t_recv, a_send, a_recv, enter,
):
    occ, vir, aux = lax.axis_index("occ"), lax.axis_index("vir"), lax.axis_index("aux")
    pairs, cols, virt = amp.shape
    nq, _, rows, bq = rbuf.shape
    block_b = bq // QC
    block_a = left.shape[0]
    cq, depth = tau.shape[3], tau.shape[4]
    pall = no * pairs
    steps = cols // CC
    subs = cq // CC
    groups = CC // 8
    half = pall * 8
    pieces = min(4, pairs)
    pp = pairs // pieces
    waves = list(range(1, nv))
    lead = max(3, nv - 2)

    place = {"occ": (occ, no), "vir": (vir, nv), "aux": (aux, na)}

    def greet(sem, axes):
        count = 0
        for axis in axes:
            at, size = place[axis]
            for k in range(1, size):
                pl.semaphore_signal(
                    sem, inc=1, device_id={axis: lax.rem(at + k, size)}, device_id_type=MESH
                )
                count += 1
        return count

    greeted = greet(pltpu.get_barrier_semaphore(), ("occ", "vir", "aux"))
    raw_copy = pltpu.make_async_copy(right_hbm, raw, raw_sem)
    raw_copy.start()
    amp_copy = pltpu.make_async_copy(amp_hbm, amp, amp_sem)
    amp_copy.start()

    def right_copy(u, n, down):
        return pltpu.make_async_remote_copy(
            src_ref=rbuf.at[n, u],
            dst_ref=rbuf.at[n, u],
            send_sem=r_send.at[1 if down else 0, u, n],
            recv_sem=r_recv.at[u, n],
            device_id={"vir": vir - 1 if down else vir + 1},
            device_id_type=MESH,
        )

    def send_own(n):
        @pl.when(vir > 0)
        def _():
            right_copy(vir, n, True).start()

        @pl.when(vir < nv - 1)
        def _():
            right_copy(vir, n, False).start()

    def arrive(k, n, forwarded, valid=True):
        for down in (True, False):
            u = vir + k if down else vir - k
            here = u < nv if down else u >= 0
            passes = vir > 0 if down else vir < nv - 1

            @pl.when(here & (passes if forwarded else jnp.logical_not(passes)) & valid)
            def _():
                right_copy(u, n, down).wait_recv()
                if forwarded:
                    right_copy(u, n, down).start()

    def relay(k, m):
        n = m - k + 1
        if k <= nv - 2:
            if isinstance(m, int):
                if 0 <= n < nq:
                    arrive(k, n, True)
            else:
                arrive(k, n, True, (n >= 0) & (n < nq))

    def more_own(m):
        n = m + AHEAD
        if isinstance(m, int):
            if n < nq:
                send_own(n)
        else:
            @pl.when(n < nq)
            def _():
                send_own(n)

    def slot(m):
        relay(1, m)
        more_own(m)
        for k in waves[1:]:
            relay(k, m)

    def left_copy(n):
        return pltpu.make_async_copy(
            left_hbm.at[:, :, pl.ds(pl.multiple_of(n * QC, QC), QC)],
            left.at[:, :, pl.ds(pl.multiple_of(n * QC, QC), QC)],
            left_sem.at[n],
        )

    sub_rows = min(rows, TILE)
    first = (occ * nv + vir) * rows

    def arrange(n, carry):
        for r in range(0, rows, sub_rows):
            m = right_mask[(first + r) // TILE, n * QC // TILE].astype(F32)
            x = raw[pl.ds(r, sub_rows), :, pl.ds(pl.multiple_of(n * QC, QC), QC)].astype(F32) * m
            for b in range(block_b):
                rbuf[n, vir, r : r + sub_rows, b * QC : (b + 1) * QC] = x[:, b, :].astype(BF16)
        return carry

    raw_copy.wait()
    lax.fori_loop(0, nq, arrange, 0)
    amp_copy.wait()
    for n in range(nq):
        left_copy(n).start()

    piece = min(cq, TILE)

    def masked(p, row, column):
        m = pair_mask[p, row // TILE, column // TILE].astype(F32)
        block = amp[
            p, pl.ds(pl.multiple_of(row, piece), piece), pl.ds(pl.multiple_of(column, TILE), TILE)
        ]
        return (block.astype(F32) * m).astype(BF16)

    def fill_send(p, carry):
        for k in range(1, no):
            base = lax.rem(occ + k, no) * depth
            for off in range(0, cq, piece):
                for col in range(0, depth, TILE):
                    tsend[k - 1, p, off : off + piece, col : col + TILE] = masked(
                        p, aux * cq + off, base + col
                    )
        return carry

    def occ_copy(k, h):
        return pltpu.make_async_remote_copy(
            src_ref=tsend.at[k - 1, pl.ds(h * pp, pp)],
            dst_ref=tau.at[occ, aux, pl.ds(h * pp, pp)],
            send_sem=t_send.at[k, 0, h],
            recv_sem=t_recv.at[occ, aux, h],
            device_id={"occ": lax.rem(occ + k, no)},
            device_id_type=MESH,
        )

    def aux_copy(k, sem, q, h, bit):
        side = lax.rem(occ + k, no)
        block = tau.at[side, q, pl.ds(h * pp, pp)]
        return pltpu.make_async_remote_copy(
            src_ref=block,
            dst_ref=block,
            send_sem=t_send.at[k, sem, h],
            recv_sem=t_recv.at[side, q, h],
            device_id={"aux": aux ^ bit},
            device_id_type=MESH,
        )

    lax.fori_loop(0, pairs, fill_send, 0)
    pl.semaphore_wait(pltpu.get_barrier_semaphore(), greeted)
    for n in range(min(AHEAD, nq)):
        send_own(n)
    tau_sends = []
    for h in range(pieces):
        for k in range(1, no):
            copy = occ_copy(k, h)
            copy.start()
            tau_sends.append(copy)

    acc[...] = jnp.zeros_like(acc)
    lhs_b[...] = jnp.zeros_like(lhs_b)
    rhs_b[...] = jnp.zeros_like(rhs_b)

    def fill_own(i, carry):
        p, q = i // na, lax.rem(i, na)
        for off in range(0, cq, piece):
            for col in range(0, depth, TILE):
                tau[occ, q, p, off : off + piece, col : col + TILE] = masked(
                    p, q * cq + off, occ * depth + col
                )
        return carry

    lax.fori_loop(0, pairs * na, fill_own, 0)

    bits = []
    bit = na // 2
    while bit:
        bits.append(bit)
        bit //= 2

    news = [[0]]
    have = [0]
    for bit in bits:
        news.append([m ^ bit for m in have])
        have = have + news[-1]
    sems = {}
    for s in range(len(news)):
        for m in news[s]:
            for later in range(s, len(bits)):
                sems[m, later] = len(sems) + 1

    def tau_stage(s, h):
        for k in range(1, no):
            for m in news[s]:
                q = aux ^ m
                aux_copy(k, 0, q, h, 0).wait_recv()
                for later in range(s, len(bits)):
                    copy = aux_copy(k, sems[m, later], q, h, bits[later])
                    copy.start()
                    tau_sends.append(copy)

    done = 0
    for w in range(pieces + len(bits)):
        for s in range(len(news)):
            if 0 <= w - s < pieces:
                tau_stage(s, w - s)
        while done < lead and (done + 1) * (pieces + len(bits)) <= (w + 1) * lead:
            slot(done)
            done += 1
    while done < lead:
        slot(done)
        done += 1
    pl.semaphore_wait(enter.at[0], greet(enter.at[0], ("vir",)))
    pl.semaphore_wait(enter.at[1], greet(enter.at[1], ("aux",)))

    def stage_two(lhs, rhs):
        acc[...] += lax.dot_general(
            lhs[...], rhs[...], (((1,), (1,)), ((), ())), preferred_element_type=F32
        )

    def stage_one(n, cs, lhs, rhs):
        c0 = pl.multiple_of(cs * CC, CC)
        q0 = pl.multiple_of(n * QC, QC)
        lm = left_mask[cs * CC // TILE, n * QC // TILE].astype(F32)
        w = left[:, pl.ds(c0, CC), pl.ds(q0, QC)].astype(F32) * lm
        w = w.reshape(block_a, groups, 8, QC)
        for j in range(groups):
            rhs[:, j * QC : (j + 1) * QC] = w[:, j].reshape(block_a * 8, QC).astype(BF16)
        q, s = cs // subs, lax.rem(cs, subs)
        t = tau[:, q, :, pl.ds(pl.multiple_of(s * CC, CC), CC), :].reshape(pall * CC, depth)
        for b in range(0, block_b, 2):
            r = rbuf[n, :, :, b * QC : (b + 2) * QC].reshape(depth, 2 * QC)
            inner = jnp.dot(t, r, preferred_element_type=F32)
            inner = inner.reshape(pall, groups, 8, 2 * QC)
            for j in range(groups):
                for e in range(2):
                    x = inner[:, j, :, e * QC : (e + 1) * QC].reshape(half, QC)
                    hi = x.astype(BF16)
                    lo = (x - hi.astype(F32)).astype(BF16)
                    row = 2 * (b + e) * half
                    lhs[row : row + half, j * QC : (j + 1) * QC] = hi
                    lhs[row + half : row + 2 * half, j * QC : (j + 1) * QC] = lo

    turns = steps // 2

    def turn(it, carry):
        n = it // turns
        ds = lax.rem(it, turns)

        @pl.when(ds == 0)
        def _():
            for k in waves:
                arrive(k, n, False)
            left_copy(n).wait()

        for k in waves[:-1]:
            @pl.when(ds == min(k, turns - 1))
            def _():
                relay(k, n + lead)
                if k == 1:
                    more_own(n + lead)

        if nv <= 2:
            @pl.when(ds == 0)
            def _():
                more_own(n + lead)

        stage_two(lhs_b, rhs_b)
        stage_one(n, 2 * ds, lhs_a, rhs_a)
        stage_two(lhs_a, rhs_a)
        stage_one(n, 2 * ds + 1, lhs_b, rhs_b)
        return carry

    lax.fori_loop(0, nq * turns, turn, 0)
    stage_two(lhs_b, rhs_b)

    width = block_a * 8
    row_i = lax.rem(lax.broadcasted_iota(jnp.int32, (half, width), 0), 8)
    col_i = lax.rem(lax.broadcasted_iota(jnp.int32, (half, width), 1), 8)
    diag = (row_i == col_i).astype(F32)
    total = jnp.zeros((pall, block_b * block_a), F32)
    src = lax.broadcasted_iota(jnp.int32, (width, block_b * block_a), 0) // 8
    dst = lax.broadcasted_iota(jnp.int32, (width, block_b * block_a), 1)
    for b in range(block_b):
        y = acc[2 * b * half : (2 * b + 1) * half, :] + acc[(2 * b + 1) * half : (2 * b + 2) * half, :]
        y = (y * diag).reshape(pall, 8, width).sum(axis=1)
        pick = (src + b * block_a == dst).astype(F32)
        total += jnp.dot(y, pick, precision=lax.Precision.HIGHEST, preferred_element_type=F32)
    part[...] = total.reshape(no, pairs, block_b * block_a)

    devices = no * nv * na
    me = (occ * nv + vir) * na + aux
    parts[me] = part[occ]

    def final_copy(k):
        j = lax.rem(me + k, devices)
        to = (j // (nv * na), lax.rem(j // na, nv), lax.rem(j, na))
        return pltpu.make_async_remote_copy(
            src_ref=part.at[to[0]],
            dst_ref=parts.at[me],
            send_sem=a_send.at[k],
            recv_sem=a_recv.at[me],
            device_id=to,
            device_id_type=MESH,
        )

    def final_arrival(k):
        j = lax.rem(me + k, devices)
        to = (j // (nv * na), lax.rem(j // na, nv), lax.rem(j, na))
        return pltpu.make_async_remote_copy(
            src_ref=part.at[to[0]],
            dst_ref=parts.at[j],
            send_sem=a_send.at[k],
            recv_sem=a_recv.at[j],
            device_id=to,
            device_id_type=MESH,
        )

    def start_final(k, carry):
        final_copy(k).start()
        return carry

    def wait_final(k, carry):
        final_arrival(k).wait_recv()
        return carry

    def drain_final(k, carry):
        final_copy(k).wait_send()
        return carry

    lax.fori_loop(1, devices, start_final, 0)
    for copy in tau_sends:
        copy.wait_send()

    def drain_right(n, carry):
        for down in (True, False):
            passes = vir > 0 if down else vir < nv - 1

            @pl.when(passes)
            def _():
                right_copy(vir, n, down).wait_send()

            for k in waves:
                u = vir + k if down else vir - k
                here = u < nv if down else u >= 0

                @pl.when(passes & here)
                def _():
                    right_copy(u, n, down).wait_send()
        return carry

    lax.fori_loop(0, nq, drain_right, 0)
    lax.fori_loop(1, devices, wait_final, 0)
    ladder = jnp.sum(parts[...], axis=0)
    for b in range(block_b):
        out[:, b, :] = res[:, b, :] + ladder[:, b * block_a : (b + 1) * block_a]
    lax.fori_loop(1, devices, drain_final, 0)


def local(sizes, amplitudes, pair_mask, left_factor, left_mask, right_factor, right_mask, residual_in):
    no, nv, na = sizes
    pairs, cols, virt = amplitudes.shape
    rows, block_b, auxn = right_factor.shape
    block_a = left_factor.shape[0]
    nq = auxn // QC
    depth = rows * nv
    cq = cols // na
    pall = no * pairs
    ba = block_b * block_a
    vmem = pl.BlockSpec(memory_space=pltpu.VMEM)
    smem = pl.BlockSpec(memory_space=pltpu.SMEM)
    hbm = pl.BlockSpec(memory_space=pltpu.MemorySpace.HBM)
    dma = pltpu.SemaphoreType.DMA
    pieces = min(4, pairs)
    depth2 = CC // 8 * QC
    return pl.pallas_call(
        functools.partial(kernel, no, nv, na),
        out_shape=jax.ShapeDtypeStruct(residual_in.shape, F32),
        in_specs=[smem, smem, smem, hbm, hbm, hbm, vmem],
        out_specs=vmem,
        scratch_shapes=[
            pltpu.VMEM(right_factor.shape, BF16),
            pltpu.VMEM((pairs, cols, virt), BF16),
            pltpu.VMEM(left_factor.shape, BF16),
            pltpu.VMEM((nq, nv, rows, block_b * QC), BF16),
            pltpu.VMEM((no, na, pairs, cq, depth), BF16),
            pltpu.VMEM((max(no - 1, 1), pairs, cq, depth), BF16),
            pltpu.VMEM((2 * block_b * pall * 8, depth2), BF16),
            pltpu.VMEM((block_a * 8, depth2), BF16),
            pltpu.VMEM((2 * block_b * pall * 8, depth2), BF16),
            pltpu.VMEM((block_a * 8, depth2), BF16),
            pltpu.VMEM((2 * block_b * pall * 8, block_a * 8), F32),
            pltpu.VMEM((no, pairs, ba), F32),
            pltpu.VMEM((no * nv * na, pairs, ba), F32),
            dma,
            dma((nq,)),
            dma,
            dma((2, nv, nq)),
            dma((nv, nq)),
            dma((no, 2 * na, pieces)),
            dma((no, na, pieces)),
            dma((no * nv * na,)),
            dma((no * nv * na,)),
            pltpu.SemaphoreType.REGULAR((2,)),
        ],
        compiler_params=pltpu.CompilerParams(
            collective_id=0, has_side_effects=True, vmem_limit_bytes=62 * 1024 * 1024
        ),
        name="ladder",
    )(pair_mask, left_mask, right_mask, amplitudes, left_factor, right_factor, residual_in)


def solution(mesh):
    sizes = tuple(mesh.shape[name] for name in ("occ", "vir", "aux"))
    return jax.shard_map(
        functools.partial(local, sizes),
        mesh=mesh,
        in_specs=(
            P("occ", "vir", None),
            P("occ", "vir", None),
            P(None, "vir", "aux"),
            P("vir", "aux"),
            P(("occ", "vir"), None, "aux"),
            P(None, "aux"),
            P("occ", None, None),
        ),
        out_specs=P("occ", None, None),
        check_vma=False,
    )
```

```python
import functools

import jax
import jax.numpy as jnp
from jax import lax
from jax.experimental import pallas as pl
from jax.experimental.pallas import tpu as pltpu
from jax.sharding import PartitionSpec as P

TILE = 128
QC = 128
CC = 64
BB = 2
AHEAD = 6
MESH = pl.DeviceIdType.MESH
F32 = jnp.float32
BF16 = jnp.bfloat16


def kernel(
    no, nv, na, pair_hbm, lmask_hbm, rmask_hbm, amp_hbm, left_hbm, right_hbm, res_hbm,
    out, pair_mask, left_mask, right_mask, res, pick, raw, amp, left, rbuf, tau, tsend, rhs, lhs_a, lhs_b, acc, part, parts,
    small_sem, amp_sem, left_sem, raw_sem, r_send, r_recv, t_send, t_recv, a_send, a_recv, enter,
):
    occ, vir, aux = lax.axis_index("occ"), lax.axis_index("vir"), lax.axis_index("aux")
    pairs, cols, virt = amp.shape
    nch, _, rows, bq = rbuf.shape
    block_b = raw.shape[1]
    nbp = block_b // BB
    nq = nch // nbp
    block_a = left.shape[0]
    cq, depth = tau.shape[3], tau.shape[4]
    pall = no * pairs
    cc = min(CC, cq)
    steps = cols // cc
    subs = cq // cc
    groups = cc // 8
    half = pall * 8
    pieces = min(4, pairs)
    pp = pairs // pieces
    waves = list(range(1, nv))
    lead = max(6, nv - 2)

    place = {"occ": (occ, no), "vir": (vir, nv), "aux": (aux, na)}

    def greet(sem, axes):
        count = 0
        for axis in axes:
            at, size = place[axis]
            for k in range(1, size):
                pl.semaphore_signal(
                    sem, inc=1, device_id={axis: lax.rem(at + k, size)}, device_id_type=MESH
                )
                count += 1
        return count

    def reach(sem, d):
        for ok, to in ((vir >= d, vir - d), (vir + d < nv, vir + d)):
            @pl.when(ok)
            def _():
                pl.semaphore_signal(sem, inc=1, device_id={"vir": to}, device_id_type=MESH)
        return (vir >= d).astype(jnp.int32) + (vir + d < nv).astype(jnp.int32)

    barrier = pltpu.get_barrier_semaphore()
    greeted = greet(barrier, ("occ", "aux")) + reach(barrier, 1)
    spans = [1 << i for i in range((nv - 1).bit_length())]
    rounds = [functools.partial(reach, d=d) for d in spans]
    rounds.append(functools.partial(greet, axes=("aux",)))
    owed = []

    def next_round():
        i = len(owed)
        if i:
            pl.semaphore_wait(enter.at[i - 1], owed[i - 1])
        if i < len(rounds):
            owed.append(rounds[i](enter.at[i]))
        elif i == len(rounds):
            owed.append(None)

    smalls = [
        pltpu.make_async_copy(*pair, small_sem.at[i])
        for i, pair in enumerate(
            ((rmask_hbm, right_mask), (pair_hbm, pair_mask), (lmask_hbm, left_mask), (res_hbm, res))
        )
    ]
    for copy in smalls[:2]:
        copy.start()
    raw_copy = pltpu.make_async_copy(right_hbm, raw, raw_sem)
    raw_copy.start()
    amp_copy = pltpu.make_async_copy(amp_hbm, amp, amp_sem)
    amp_copy.start()
    for copy in smalls[2:]:
        copy.start()

    def right_copy(u, n, down):
        return pltpu.make_async_remote_copy(
            src_ref=rbuf.at[n, u],
            dst_ref=rbuf.at[n, u],
            send_sem=r_send.at[1 if down else 0, u, n],
            recv_sem=r_recv.at[u, n],
            device_id={"vir": vir - 1 if down else vir + 1},
            device_id_type=MESH,
        )

    def send_own(n):
        @pl.when(vir > 0)
        def _():
            right_copy(vir, n, True).start()

        @pl.when(vir < nv - 1)
        def _():
            right_copy(vir, n, False).start()

    def arrive(k, n, forwarded, valid=True):
        for down in (True, False):
            u = vir + k if down else vir - k
            here = u < nv if down else u >= 0
            passes = vir > 0 if down else vir < nv - 1

            @pl.when(here & (passes if forwarded else jnp.logical_not(passes)) & valid)
            def _():
                right_copy(u, n, down).wait_recv()
                if forwarded:
                    right_copy(u, n, down).start()

    def relay(k, m):
        n = m - k + 1
        if k <= nv - 2:
            if isinstance(m, int):
                if 0 <= n < nch:
                    arrive(k, n, True)
            else:
                arrive(k, n, True, (n >= 0) & (n < nch))

    def more_own(m):
        n = m + AHEAD
        if isinstance(m, int):
            if n < nch:
                send_own(n)
        else:
            @pl.when(n < nch)
            def _():
                send_own(n)

    def slot(m):
        relay(1, m)
        more_own(m)
        for k in waves[1:]:
            relay(k, m)

    def left_copy(n):
        return pltpu.make_async_copy(
            left_hbm.at[:, :, pl.ds(pl.multiple_of(n * QC, QC), QC)],
            left.at[:, :, pl.ds(pl.multiple_of(n * QC, QC), QC)],
            left_sem.at[n],
        )

    sub_rows = min(rows, TILE)
    first = (occ * nv + vir) * rows

    def arrange(n, carry):
        for r in range(0, rows, sub_rows):
            m = right_mask[(first + r) // TILE, n * QC // TILE].astype(F32)
            x = raw[pl.ds(r, sub_rows), :, pl.ds(pl.multiple_of(n * QC, QC), QC)].astype(F32) * m
            for b in range(block_b):
                j, e = n * nbp + b // BB, b % BB
                rbuf[j, vir, r : r + sub_rows, e * QC : (e + 1) * QC] = x[:, b, :].astype(BF16)
        return carry

    smalls[0].wait()
    raw_copy.wait()
    lax.fori_loop(0, nq, arrange, 0)
    smalls[1].wait()
    amp_copy.wait()
    for n in range(nq):
        left_copy(n).start()

    piece = min(cq, TILE)

    def masked(p, row, column):
        m = pair_mask[p, row // TILE, column // TILE].astype(F32)
        block = amp[
            p, pl.ds(pl.multiple_of(row, piece), piece), pl.ds(pl.multiple_of(column, TILE), TILE)
        ]
        return (block.astype(F32) * m).astype(BF16)

    def fill_send(p, carry):
        for k in range(1, no):
            base = lax.rem(occ + k, no) * depth
            for off in range(0, cq, piece):
                for col in range(0, depth, TILE):
                    tsend[k - 1, p, off : off + piece, col : col + TILE] = masked(
                        p, aux * cq + off, base + col
                    )
        return carry

    def occ_copy(k, h):
        return pltpu.make_async_remote_copy(
            src_ref=tsend.at[k - 1, pl.ds(h * pp, pp)],
            dst_ref=tau.at[occ, aux, pl.ds(h * pp, pp)],
            send_sem=t_send.at[k, 0, h],
            recv_sem=t_recv.at[occ, aux, h],
            device_id={"occ": lax.rem(occ + k, no)},
            device_id_type=MESH,
        )

    def aux_copy(k, sem, q, h, bit):
        side = lax.rem(occ + k, no)
        block = tau.at[side, q, pl.ds(h * pp, pp)]
        return pltpu.make_async_remote_copy(
            src_ref=block,
            dst_ref=block,
            send_sem=t_send.at[k, sem, h],
            recv_sem=t_recv.at[side, q, h],
            device_id={"aux": aux ^ bit},
            device_id_type=MESH,
        )

    lax.fori_loop(0, pairs, fill_send, 0)
    pl.semaphore_wait(barrier, greeted)
    for n in range(min(AHEAD, nch)):
        send_own(n)
    tau_sends = []
    for h in range(pieces):
        for k in range(1, no):
            copy = occ_copy(k, h)
            copy.start()
            tau_sends.append(copy)
    next_round()

    ba = block_b * block_a
    wide = block_b * block_a * 8
    src = lax.broadcasted_iota(jnp.int32, (wide, ba), 0) // 8
    dst = lax.broadcasted_iota(jnp.int32, (wide, ba), 1)
    pick[...] = (src == dst).astype(F32).astype(BF16)
    acc[...] = jnp.zeros_like(acc)
    lhs_b[...] = jnp.zeros_like(lhs_b)

    def fill_own(i, carry):
        p, q = i // na, lax.rem(i, na)
        for off in range(0, cq, piece):
            for col in range(0, depth, TILE):
                tau[occ, q, p, off : off + piece, col : col + TILE] = masked(
                    p, q * cq + off, occ * depth + col
                )
        return carry

    lax.fori_loop(0, pairs * na, fill_own, 0)

    bits = []
    bit = na // 2
    while bit:
        bits.append(bit)
        bit //= 2

    news = [[0]]
    have = [0]
    for bit in bits:
        news.append([m ^ bit for m in have])
        have = have + news[-1]
    sems = {}
    for s in range(len(news)):
        for m in news[s]:
            for later in range(s, len(bits)):
                sems[m, later] = len(sems) + 1

    def tau_stage(s, h):
        for k in range(1, no):
            for m in news[s]:
                q = aux ^ m
                aux_copy(k, 0, q, h, 0).wait_recv()
                for later in range(s, len(bits)):
                    copy = aux_copy(k, sems[m, later], q, h, bits[later])
                    copy.start()
                    tau_sends.append(copy)

    def prepare(i, carry):
        n, cs = i // steps, lax.rem(i, steps)

        @pl.when(cs == 0)
        def _():
            left_copy(n).wait()

        c0 = pl.multiple_of(cs * cc, cc)
        q0 = pl.multiple_of(n * QC, QC)
        lm = left_mask[cs * cc // TILE, n * QC // TILE].astype(F32)
        w = left[:, pl.ds(c0, cc), pl.ds(q0, QC)].astype(F32) * lm
        w = w.reshape(block_a, groups, 8, QC)
        for j in range(groups):
            rhs[i, :, j * QC : (j + 1) * QC] = w[:, j].reshape(block_a * 8, QC).astype(BF16)
        return carry

    smalls[2].wait()
    ready = 0
    done = 0
    for w in range(pieces + len(bits)):
        for s in range(len(news)):
            if 0 <= w - s < pieces:
                tau_stage(s, w - s)
        while done < lead and (done + 1) * (pieces + len(bits)) <= (w + 1) * lead:
            slot(done)
            done += 1
        if 0 < w <= len(rounds):
            next_round()
        upto = nq * steps * (w + 1) // (pieces + len(bits))
        lax.fori_loop(ready, upto, prepare, 0)
        ready = upto
    while done < lead:
        slot(done)
        done += 1
    while len(owed) <= len(rounds):
        next_round()
    lax.fori_loop(ready, nq * steps, prepare, 0)

    def stage_two(e, lhs, i):
        span = pl.ds(pl.multiple_of(e * (2 * BB * half), 2 * BB * half), 2 * BB * half)
        acc[span, :] += lax.dot_general(
            lhs[...], rhs[i], (((1,), (1,)), ((), ())), preferred_element_type=F32
        )

    def stage_one(ch, cs, lhs):
        q, s = cs // subs, lax.rem(cs, subs)
        t = tau[:, q, :, pl.ds(pl.multiple_of(s * cc, cc), cc), :].reshape(pall * cc, depth)
        r = rbuf[ch].reshape(depth, bq)
        inner = jnp.dot(t, r, preferred_element_type=F32)
        inner = inner.reshape(pall, groups, 8, bq)
        for j in range(groups):
            for e in range(BB):
                x = inner[:, j, :, e * QC : (e + 1) * QC].reshape(half, QC)
                hi = x.astype(BF16)
                lo = (x - hi.astype(F32)).astype(BF16)
                row = 2 * e * half
                lhs[row : row + half, j * QC : (j + 1) * QC] = hi
                lhs[row + half : row + 2 * half, j * QC : (j + 1) * QC] = lo

    turns = steps // 2

    def turn(it, carry):
        ch = it // turns
        ds = lax.rem(it, turns)
        n, e = ch // nbp, lax.rem(ch, nbp)

        @pl.when(ds == 0)
        def _():
            for k in waves:
                arrive(k, ch, False)

        @pl.when(ds == turns - 1)
        def _():
            slot(ch + lead)

        last = jnp.maximum(it - 1, 0) // turns
        back = jnp.where(ds == 0, last // nbp * steps + steps - 1, n * steps + 2 * ds - 1)
        stage_one(ch, 2 * ds, lhs_a)
        stage_two(lax.rem(last, nbp), lhs_b, back)
        stage_one(ch, 2 * ds + 1, lhs_b)
        stage_two(e, lhs_a, n * steps + 2 * ds)
        return carry

    lax.fori_loop(0, nch * turns, turn, 0)
    stage_two(nbp - 1, lhs_b, nq * steps - 1)

    width = block_a * 8
    row_i = lax.rem(lax.broadcasted_iota(jnp.int32, (half, width), 0), 8)
    col_i = lax.rem(lax.broadcasted_iota(jnp.int32, (half, width), 1), 8)
    diag = (row_i == col_i).astype(F32)
    total = jnp.zeros((pall, ba), F32)
    for b in range(block_b):
        y = acc[2 * b * half : (2 * b + 1) * half, :] + acc[(2 * b + 1) * half : (2 * b + 2) * half, :]
        y = (y * diag).reshape(pall, 8, width).sum(axis=1)
        for _ in range(3):
            z = y.astype(BF16)
            total += jnp.dot(
                z, pick[b * width : (b + 1) * width, :], preferred_element_type=F32
            )
            y = y - z.astype(F32)
    part[...] = total.reshape(no, pairs, ba)

    devices = no * nv * na
    me = (occ * nv + vir) * na + aux
    parts[me] = part[occ]

    def final_copy(k):
        j = lax.rem(me + k, devices)
        to = (j // (nv * na), lax.rem(j // na, nv), lax.rem(j, na))
        return pltpu.make_async_remote_copy(
            src_ref=part.at[to[0]],
            dst_ref=parts.at[me],
            send_sem=a_send.at[k],
            recv_sem=a_recv.at[me],
            device_id=to,
            device_id_type=MESH,
        )

    def final_arrival(k):
        j = lax.rem(me + k, devices)
        to = (j // (nv * na), lax.rem(j // na, nv), lax.rem(j, na))
        return pltpu.make_async_remote_copy(
            src_ref=part.at[to[0]],
            dst_ref=parts.at[j],
            send_sem=a_send.at[k],
            recv_sem=a_recv.at[j],
            device_id=to,
            device_id_type=MESH,
        )

    def start_final(k, carry):
        final_copy(k).start()
        return carry

    def wait_final(k, carry):
        final_arrival(k).wait_recv()
        return carry

    def drain_final(k, carry):
        final_copy(k).wait_send()
        return carry

    lax.fori_loop(1, devices, start_final, 0)
    for copy in tau_sends:
        copy.wait_send()

    def drain_right(n, carry):
        for down in (True, False):
            passes = vir > 0 if down else vir < nv - 1

            @pl.when(passes)
            def _():
                right_copy(vir, n, down).wait_send()

            for k in waves:
                u = vir + k if down else vir - k
                here = u < nv if down else u >= 0

                @pl.when(passes & here)
                def _():
                    right_copy(u, n, down).wait_send()
        return carry

    lax.fori_loop(0, nch, drain_right, 0)
    lax.fori_loop(1, devices, wait_final, 0)
    smalls[3].wait()
    ladder = jnp.sum(parts[...], axis=0)
    for b in range(block_b):
        out[:, b, :] = res[:, b, :] + ladder[:, b * block_a : (b + 1) * block_a]
    lax.fori_loop(1, devices, drain_final, 0)


def local(sizes, amplitudes, pair_mask, left_factor, left_mask, right_factor, right_mask, residual_in):
    no, nv, na = sizes
    pairs, cols, virt = amplitudes.shape
    rows, block_b, auxn = right_factor.shape
    block_a = left_factor.shape[0]
    nq = auxn // QC
    nch = nq * block_b // BB
    depth = rows * nv
    cq = cols // na
    pall = no * pairs
    ba = block_b * block_a
    vmem = pl.BlockSpec(memory_space=pltpu.VMEM)
    hbm = pl.BlockSpec(memory_space=pltpu.MemorySpace.HBM)
    dma = pltpu.SemaphoreType.DMA
    pieces = min(4, pairs)
    inner = min(CC, cq) // 8 * QC
    return pl.pallas_call(
        functools.partial(kernel, no, nv, na),
        out_shape=jax.ShapeDtypeStruct(residual_in.shape, F32),
        in_specs=[hbm] * 7,
        out_specs=vmem,
        scratch_shapes=[
            pltpu.SMEM(pair_mask.shape, jnp.int32),
            pltpu.SMEM(left_mask.shape, jnp.int32),
            pltpu.SMEM(right_mask.shape, jnp.int32),
            pltpu.VMEM(residual_in.shape, F32),
            pltpu.VMEM((ba * 8, ba), BF16),
            pltpu.VMEM(right_factor.shape, BF16),
            pltpu.VMEM((pairs, cols, virt), BF16),
            pltpu.VMEM(left_factor.shape, BF16),
            pltpu.VMEM((nch, nv, rows, BB * QC), BF16),
            pltpu.VMEM((no, na, pairs, cq, depth), BF16),
            pltpu.VMEM((max(no - 1, 1), pairs, cq, depth), BF16),
            pltpu.VMEM((nq * cols // min(CC, cq), block_a * 8, inner), BF16),
            pltpu.VMEM((2 * BB * pall * 8, inner), BF16),
            pltpu.VMEM((2 * BB * pall * 8, inner), BF16),
            pltpu.VMEM((2 * block_b * pall * 8, block_a * 8), F32),
            pltpu.VMEM((no, pairs, ba), F32),
            pltpu.VMEM((no * nv * na, pairs, ba), F32),
            dma((4,)),
            dma,
            dma((nq,)),
            dma,
            dma((2, nv, nch)),
            dma((nv, nch)),
            dma((no, 2 * na, pieces)),
            dma((no, na, pieces)),
            dma((no * nv * na,)),
            dma((no * nv * na,)),
            pltpu.SemaphoreType.REGULAR((nv.bit_length() + 1,)),
        ],
        compiler_params=pltpu.CompilerParams(
            collective_id=0, has_side_effects=True, vmem_limit_bytes=62 * 1024 * 1024
        ),
        name="ladder",
    )(pair_mask, left_mask, right_mask, amplitudes, left_factor, right_factor, residual_in)


def solution(mesh):
    sizes = tuple(mesh.shape[name] for name in ("occ", "vir", "aux"))
    return jax.shard_map(
        functools.partial(local, sizes),
        mesh=mesh,
        in_specs=(
            P("occ", "vir", None),
            P("occ", "vir", None),
            P(None, "vir", "aux"),
            P("vir", "aux"),
            P(("occ", "vir"), None, "aux"),
            P(None, "aux"),
            P("occ", None, None),
        ),
        out_specs=P("occ", None, None),
        check_vma=False,
    )
```

```python
import functools

import jax
import jax.numpy as jnp
from jax import lax
from jax.experimental import pallas as pl
from jax.experimental.pallas import tpu as pltpu
from jax.sharding import PartitionSpec as P

TILE = 128
QC = 128
CC = 64
BB = 2
AHEAD = 4
MESH = pl.DeviceIdType.MESH
F32 = jnp.float32
BF16 = jnp.bfloat16


def kernel(
    no, nv, na, pair_hbm, lmask_hbm, rmask_hbm, amp_hbm, left_hbm, right_hbm, res_hbm,
    out, pair_mask, left_mask, right_mask, res, pick, raw, amp, left, rbuf, tau, tsend, rhs, lhs_a, lhs_b, acc, part, parts,
    small_sem, amp_sem, left_sem, raw_sem, r_send, r_recv, t_send, t_recv, a_send, a_recv, enter,
):
    occ, vir, aux = lax.axis_index("occ"), lax.axis_index("vir"), lax.axis_index("aux")
    pairs, cols, virt = amp.shape
    nq, _, nbp, rows, bq = rbuf.shape
    block_b = raw.shape[1]
    nch = nq * nbp
    units = nq - 1 + nbp
    block_a = left.shape[0]
    cq, depth = tau.shape[3], tau.shape[4]
    pall = no * pairs
    cc = min(CC, cq)
    steps = cols // cc
    subs = cq // cc
    groups = cc // 8
    half = pall * 8
    pieces = min(4, pairs)
    pp = pairs // pieces
    waves = list(range(1, nv))
    lead = max(3, nv - 2)

    place = {"occ": (occ, no), "vir": (vir, nv), "aux": (aux, na)}

    def greet(sem, axes):
        count = 0
        for axis in axes:
            at, size = place[axis]
            for k in range(1, size):
                pl.semaphore_signal(
                    sem, inc=1, device_id={axis: lax.rem(at + k, size)}, device_id_type=MESH
                )
                count += 1
        return count

    def reach(sem, d):
        for ok, to in ((vir >= d, vir - d), (vir + d < nv, vir + d)):
            @pl.when(ok)
            def _():
                pl.semaphore_signal(sem, inc=1, device_id={"vir": to}, device_id_type=MESH)
        return (vir >= d).astype(jnp.int32) + (vir + d < nv).astype(jnp.int32)

    barrier = pltpu.get_barrier_semaphore()
    greeted = greet(barrier, ("occ", "aux")) + reach(barrier, 1)
    spans = [1 << i for i in range((nv - 1).bit_length())]
    rounds = [functools.partial(reach, d=d) for d in spans]
    rounds.append(functools.partial(greet, axes=("aux",)))
    owed = []

    def next_round():
        i = len(owed)
        if i:
            pl.semaphore_wait(enter.at[i - 1], owed[i - 1])
        if i < len(rounds):
            owed.append(rounds[i](enter.at[i]))
        elif i == len(rounds):
            owed.append(None)

    smalls = [
        pltpu.make_async_copy(*pair, small_sem.at[i])
        for i, pair in enumerate(
            ((rmask_hbm, right_mask), (pair_hbm, pair_mask), (lmask_hbm, left_mask), (res_hbm, res))
        )
    ]
    for copy in smalls[:2]:
        copy.start()
    raw_copy = pltpu.make_async_copy(right_hbm, raw, raw_sem)
    raw_copy.start()
    amp_copy = pltpu.make_async_copy(amp_hbm, amp, amp_sem)
    amp_copy.start()
    for copy in smalls[2:]:
        copy.start()

    def right_copy(u, m, down, big):
        block = rbuf.at[m, u] if big else rbuf.at[nq - 1, u, m - (nq - 1)]
        return pltpu.make_async_remote_copy(
            src_ref=block,
            dst_ref=block,
            send_sem=r_send.at[1 if down else 0, u, m],
            recv_sem=r_recv.at[u, m],
            device_id={"vir": vir - 1 if down else vir + 1},
            device_id_type=MESH,
        )

    def sized(m, act, ok=True):
        if isinstance(m, int):
            if 0 <= m < units:
                act(m < nq - 1)
            return

        @pl.when(ok & (m >= 0) & (m < nq - 1))
        def _():
            act(True)

        @pl.when(ok & (m >= nq - 1) & (m < units))
        def _():
            act(False)

    def send_own(m):
        def act(big):
            @pl.when(vir > 0)
            def _():
                right_copy(vir, m, True, big).start()

            @pl.when(vir < nv - 1)
            def _():
                right_copy(vir, m, False, big).start()

        sized(m, act)

    def arrive(k, m, forwarded, ok=True):
        def act(big):
            for down in (True, False):
                u = vir + k if down else vir - k
                here = u < nv if down else u >= 0
                passes = vir > 0 if down else vir < nv - 1

                @pl.when(here & (passes if forwarded else jnp.logical_not(passes)))
                def _():
                    right_copy(u, m, down, big).wait_recv()
                    if forwarded:
                        right_copy(u, m, down, big).start()

        sized(m, act, ok)

    def slot(m):
        for k in reversed(waves[:-1]):
            arrive(k, m - k + 1, True, (vir > 0) & (vir < nv - 1))
        if isinstance(m, int):
            if m == 0:
                send_own(AHEAD)
            elif m % 2:
                send_own(AHEAD + (m + 1) // 2)
        else:
            @pl.when(lax.rem(m, 2) == 1)
            def _():
                send_own(AHEAD + (m + 1) // 2)

    def left_copy(n):
        return pltpu.make_async_copy(
            left_hbm.at[:, :, pl.ds(pl.multiple_of(n * QC, QC), QC)],
            left.at[:, :, pl.ds(pl.multiple_of(n * QC, QC), QC)],
            left_sem.at[n],
        )

    sub_rows = min(rows, TILE)
    first = (occ * nv + vir) * rows

    def arrange(n, carry):
        for r in range(0, rows, sub_rows):
            m = right_mask[(first + r) // TILE, n * QC // TILE].astype(F32)
            x = raw[pl.ds(r, sub_rows), :, pl.ds(pl.multiple_of(n * QC, QC), QC)].astype(F32) * m
            for b in range(block_b):
                e = b % BB
                rbuf[n, vir, b // BB, r : r + sub_rows, e * QC : (e + 1) * QC] = x[:, b, :].astype(
                    BF16
                )
        return carry

    smalls[0].wait()
    raw_copy.wait()
    lax.fori_loop(0, nq, arrange, 0)
    smalls[1].wait()
    amp_copy.wait()
    for n in range(nq):
        left_copy(n).start()

    piece = min(cq, TILE)

    def masked(p, row, column):
        m = pair_mask[p, row // TILE, column // TILE].astype(F32)
        block = amp[
            p, pl.ds(pl.multiple_of(row, piece), piece), pl.ds(pl.multiple_of(column, TILE), TILE)
        ]
        return (block.astype(F32) * m).astype(BF16)

    def fill_send(p, carry):
        for k in range(1, no):
            base = lax.rem(occ + k, no) * depth
            for off in range(0, cq, piece):
                for col in range(0, depth, TILE):
                    tsend[k - 1, p, off : off + piece, col : col + TILE] = masked(
                        p, aux * cq + off, base + col
                    )
        return carry

    def occ_copy(k, h):
        return pltpu.make_async_remote_copy(
            src_ref=tsend.at[k - 1, pl.ds(h * pp, pp)],
            dst_ref=tau.at[occ, aux, pl.ds(h * pp, pp)],
            send_sem=t_send.at[k, 0, h],
            recv_sem=t_recv.at[occ, aux, h],
            device_id={"occ": lax.rem(occ + k, no)},
            device_id_type=MESH,
        )

    def aux_copy(k, sem, q, h, bit):
        side = lax.rem(occ + k, no)
        block = tau.at[side, q, pl.ds(h * pp, pp)]
        return pltpu.make_async_remote_copy(
            src_ref=block,
            dst_ref=block,
            send_sem=t_send.at[k, sem, h],
            recv_sem=t_recv.at[side, q, h],
            device_id={"aux": aux ^ bit},
            device_id_type=MESH,
        )

    lax.fori_loop(0, pairs, fill_send, 0)
    pl.semaphore_wait(barrier, greeted)
    for n in range(AHEAD):
        send_own(n)
    tau_sends = []
    for h in range(pieces):
        for k in range(1, no):
            copy = occ_copy(k, h)
            copy.start()
            tau_sends.append(copy)
    next_round()

    ba = block_b * block_a
    wide = block_b * block_a * 8
    src = lax.broadcasted_iota(jnp.int32, (wide, ba), 0) // 8
    dst = lax.broadcasted_iota(jnp.int32, (wide, ba), 1)
    pick[...] = (src == dst).astype(F32).astype(BF16)
    acc[...] = jnp.zeros_like(acc)
    lhs_b[...] = jnp.zeros_like(lhs_b)

    def fill_own(i, carry):
        p, q = i // na, lax.rem(i, na)
        for off in range(0, cq, piece):
            for col in range(0, depth, TILE):
                tau[occ, q, p, off : off + piece, col : col + TILE] = masked(
                    p, q * cq + off, occ * depth + col
                )
        return carry

    lax.fori_loop(0, pairs * na, fill_own, 0)

    bits = []
    bit = na // 2
    while bit:
        bits.append(bit)
        bit //= 2

    news = [[0]]
    have = [0]
    for bit in bits:
        news.append([m ^ bit for m in have])
        have = have + news[-1]
    sems = {}
    for s in range(len(news)):
        for m in news[s]:
            for later in range(s, len(bits)):
                sems[m, later] = len(sems) + 1

    def tau_stage(s, h):
        for k in range(1, no):
            for m in news[s]:
                q = aux ^ m
                aux_copy(k, 0, q, h, 0).wait_recv()
                for later in range(s, len(bits)):
                    copy = aux_copy(k, sems[m, later], q, h, bits[later])
                    copy.start()
                    tau_sends.append(copy)

    def prepare(i, carry):
        n, cs = i // steps, lax.rem(i, steps)

        @pl.when(cs == 0)
        def _():
            left_copy(n).wait()

        c0 = pl.multiple_of(cs * cc, cc)
        q0 = pl.multiple_of(n * QC, QC)
        lm = left_mask[cs * cc // TILE, n * QC // TILE].astype(F32)
        w = left[:, pl.ds(c0, cc), pl.ds(q0, QC)].astype(F32) * lm
        w = w.reshape(block_a, groups, 8, QC)
        for j in range(groups):
            rhs[i, :, j * QC : (j + 1) * QC] = w[:, j].reshape(block_a * 8, QC).astype(BF16)
        return carry

    smalls[2].wait()
    ready = 0
    done = 0
    for w in range(pieces + len(bits)):
        for s in range(len(news)):
            if 0 <= w - s < pieces:
                tau_stage(s, w - s)
        while done < lead and (done + 1) * (pieces + len(bits)) <= (w + 1) * lead:
            slot(done)
            done += 1
        if 0 < w <= len(rounds):
            next_round()
        upto = nq * steps * (w + 1) // (pieces + len(bits))
        lax.fori_loop(ready, upto, prepare, 0)
        ready = upto
    while done < lead:
        slot(done)
        done += 1
    while len(owed) <= len(rounds):
        next_round()
    lax.fori_loop(ready, nq * steps, prepare, 0)

    def stage_two(e, lhs, i):
        span = pl.ds(pl.multiple_of(e * (2 * BB * half), 2 * BB * half), 2 * BB * half)
        acc[span, :] += lax.dot_general(
            lhs[...], rhs[i], (((1,), (1,)), ((), ())), preferred_element_type=F32
        )

    def stage_one(n, e, cs, lhs):
        q, s = cs // subs, lax.rem(cs, subs)
        t = tau[:, q, :, pl.ds(pl.multiple_of(s * cc, cc), cc), :].reshape(pall * cc, depth)
        r = rbuf[n, :, e].reshape(depth, bq)
        inner = jnp.dot(t, r, preferred_element_type=F32)
        inner = inner.reshape(pall, groups, 8, bq)
        for j in range(groups):
            for e in range(BB):
                x = inner[:, j, :, e * QC : (e + 1) * QC].reshape(half, QC)
                hi = x.astype(BF16)
                lo = (x - hi.astype(F32)).astype(BF16)
                row = 2 * e * half
                lhs[row : row + half, j * QC : (j + 1) * QC] = hi
                lhs[row + half : row + 2 * half, j * QC : (j + 1) * QC] = lo

    def chunk(ch, carry):
        n, e = ch // nbp, lax.rem(ch, nbp)
        ending = n == nq - 1
        unit = jnp.where(ending, nq - 1 + e, n)

        @pl.when(ending | (e == 0))
        def _():
            for k in waves:
                arrive(k, unit, False)

        @pl.when((ending | (e == nbp - 1)) & (unit + lead < units + nv - 3))
        def _():
            slot(unit + lead)

        last = jnp.maximum(ch - 1, 0)
        for cs in range(steps):
            now, old = (lhs_a, lhs_b) if cs % 2 == 0 else (lhs_b, lhs_a)
            stage_one(n, e, cs, now)
            if cs == 0:
                stage_two(lax.rem(last, nbp), old, last // nbp * steps + steps - 1)
            else:
                stage_two(e, old, n * steps + cs - 1)
        return carry

    lax.fori_loop(0, nch, chunk, 0)
    stage_two(nbp - 1, lhs_b, nq * steps - 1)

    width = block_a * 8
    row_i = lax.rem(lax.broadcasted_iota(jnp.int32, (half, width), 0), 8)
    col_i = lax.rem(lax.broadcasted_iota(jnp.int32, (half, width), 1), 8)
    diag = (row_i == col_i).astype(F32)
    total = jnp.zeros((pall, ba), F32)
    for b in range(block_b):
        y = acc[2 * b * half : (2 * b + 1) * half, :] + acc[(2 * b + 1) * half : (2 * b + 2) * half, :]
        y = (y * diag).reshape(pall, 8, width).sum(axis=1)
        for _ in range(3):
            z = y.astype(BF16)
            total += jnp.dot(
                z, pick[b * width : (b + 1) * width, :], preferred_element_type=F32
            )
            y = y - z.astype(F32)
    part[...] = total.reshape(no, pairs, ba)

    devices = no * nv * na
    me = (occ * nv + vir) * na + aux
    parts[me] = part[occ]

    def final_copy(k):
        j = lax.rem(me + k, devices)
        to = (j // (nv * na), lax.rem(j // na, nv), lax.rem(j, na))
        return pltpu.make_async_remote_copy(
            src_ref=part.at[to[0]],
            dst_ref=parts.at[me],
            send_sem=a_send.at[k],
            recv_sem=a_recv.at[me],
            device_id=to,
            device_id_type=MESH,
        )

    def final_arrival(k):
        j = lax.rem(me + k, devices)
        to = (j // (nv * na), lax.rem(j // na, nv), lax.rem(j, na))
        return pltpu.make_async_remote_copy(
            src_ref=part.at[to[0]],
            dst_ref=parts.at[j],
            send_sem=a_send.at[k],
            recv_sem=a_recv.at[j],
            device_id=to,
            device_id_type=MESH,
        )

    def start_final(k, carry):
        final_copy(k).start()
        return carry

    def wait_final(k, carry):
        final_arrival(k).wait_recv()
        return carry

    def drain_final(k, carry):
        final_copy(k).wait_send()
        return carry

    lax.fori_loop(1, devices, start_final, 0)
    for copy in tau_sends:
        copy.wait_send()

    def drain_right(m, carry):
        def act(big):
            for down in (True, False):
                passes = vir > 0 if down else vir < nv - 1

                @pl.when(passes)
                def _():
                    right_copy(vir, m, down, big).wait_send()

                for k in waves:
                    u = vir + k if down else vir - k
                    here = u < nv if down else u >= 0

                    @pl.when(passes & here)
                    def _():
                        right_copy(u, m, down, big).wait_send()

        sized(m, act)
        return carry

    lax.fori_loop(0, units, drain_right, 0)
    lax.fori_loop(1, devices, wait_final, 0)
    smalls[3].wait()
    ladder = jnp.sum(parts[...], axis=0)
    for b in range(block_b):
        out[:, b, :] = res[:, b, :] + ladder[:, b * block_a : (b + 1) * block_a]
    lax.fori_loop(1, devices, drain_final, 0)


def local(sizes, amplitudes, pair_mask, left_factor, left_mask, right_factor, right_mask, residual_in):
    no, nv, na = sizes
    pairs, cols, virt = amplitudes.shape
    rows, block_b, auxn = right_factor.shape
    block_a = left_factor.shape[0]
    nq = auxn // QC
    units = nq - 1 + block_b // BB
    depth = rows * nv
    cq = cols // na
    pall = no * pairs
    ba = block_b * block_a
    vmem = pl.BlockSpec(memory_space=pltpu.VMEM)
    hbm = pl.BlockSpec(memory_space=pltpu.MemorySpace.HBM)
    dma = pltpu.SemaphoreType.DMA
    pieces = min(4, pairs)
    inner = min(CC, cq) // 8 * QC
    return pl.pallas_call(
        functools.partial(kernel, no, nv, na),
        out_shape=jax.ShapeDtypeStruct(residual_in.shape, F32),
        in_specs=[hbm] * 7,
        out_specs=vmem,
        scratch_shapes=[
            pltpu.SMEM(pair_mask.shape, jnp.int32),
            pltpu.SMEM(left_mask.shape, jnp.int32),
            pltpu.SMEM(right_mask.shape, jnp.int32),
            pltpu.VMEM(residual_in.shape, F32),
            pltpu.VMEM((ba * 8, ba), BF16),
            pltpu.VMEM(right_factor.shape, BF16),
            pltpu.VMEM((pairs, cols, virt), BF16),
            pltpu.VMEM(left_factor.shape, BF16),
            pltpu.VMEM((nq, nv, block_b // BB, rows, BB * QC), BF16),
            pltpu.VMEM((no, na, pairs, cq, depth), BF16),
            pltpu.VMEM((max(no - 1, 1), pairs, cq, depth), BF16),
            pltpu.VMEM((nq * cols // min(CC, cq), block_a * 8, inner), BF16),
            pltpu.VMEM((2 * BB * pall * 8, inner), BF16),
            pltpu.VMEM((2 * BB * pall * 8, inner), BF16),
            pltpu.VMEM((2 * block_b * pall * 8, block_a * 8), F32),
            pltpu.VMEM((no, pairs, ba), F32),
            pltpu.VMEM((no * nv * na, pairs, ba), F32),
            dma((4,)),
            dma,
            dma((nq,)),
            dma,
            dma((2, nv, units)),
            dma((nv, units)),
            dma((no, 2 * na, pieces)),
            dma((no, na, pieces)),
            dma((no * nv * na,)),
            dma((no * nv * na,)),
            pltpu.SemaphoreType.REGULAR((nv.bit_length() + 1,)),
        ],
        compiler_params=pltpu.CompilerParams(
            collective_id=0, has_side_effects=True, vmem_limit_bytes=62 * 1024 * 1024
        ),
        name="ladder",
    )(pair_mask, left_mask, right_mask, amplitudes, left_factor, right_factor, residual_in)


def solution(mesh):
    sizes = tuple(mesh.shape[name] for name in ("occ", "vir", "aux"))
    return jax.shard_map(
        functools.partial(local, sizes),
        mesh=mesh,
        in_specs=(
            P("occ", "vir", None),
            P("occ", "vir", None),
            P(None, "vir", "aux"),
            P("vir", "aux"),
            P(("occ", "vir"), None, "aux"),
            P(None, "aux"),
            P("occ", None, None),
        ),
        out_specs=P("occ", None, None),
        check_vma=False,
    )
```

```python
import functools

import jax
import jax.numpy as jnp
from jax import lax
from jax.experimental import pallas as pl
from jax.experimental.pallas import tpu as pltpu
from jax.sharding import PartitionSpec as P

TILE = 128
QC = 128
CC = 64
BB = 2
AHEAD = 4
MESH = pl.DeviceIdType.MESH
F32 = jnp.float32
BF16 = jnp.bfloat16


def kernel(
    no, nv, na, pair_hbm, lmask_hbm, rmask_hbm, amp_hbm, left_hbm, right_hbm, res_hbm,
    out, pair_mask, left_mask, right_mask, res, pick, raw, amp, left, rbuf, tau, tsend, rhs, lhs_a, lhs_b, acc, part, parts,
    small_sem, amp_sem, left_sem, raw_sem, r_send, r_recv, t_send, t_recv, a_send, a_recv, enter,
):
    occ, vir, aux = lax.axis_index("occ"), lax.axis_index("vir"), lax.axis_index("aux")
    pairs, cols, virt = amp.shape
    nq, _, nbp, rows, bq = rbuf.shape
    block_b = raw.shape[1]
    nch = nq * nbp
    units = nq - 1 + nbp
    block_a = left.shape[0]
    cq, depth = tau.shape[3], tau.shape[4]
    pall = no * pairs
    cc = min(CC, cq)
    steps = cols // cc
    subs = cq // cc
    groups = cc // 8
    half = pall * 8
    pieces = min(4, pairs)
    pp = pairs // pieces
    waves = list(range(1, nv))
    lead = max(3, nv - 2)

    place = {"occ": (occ, no), "vir": (vir, nv), "aux": (aux, na)}

    def greet(sem, axes):
        count = 0
        for axis in axes:
            at, size = place[axis]
            for k in range(1, size):
                pl.semaphore_signal(
                    sem, inc=1, device_id={axis: lax.rem(at + k, size)}, device_id_type=MESH
                )
                count += 1
        return count

    def reach(sem, d):
        for ok, to in ((vir >= d, vir - d), (vir + d < nv, vir + d)):
            @pl.when(ok)
            def _():
                pl.semaphore_signal(sem, inc=1, device_id={"vir": to}, device_id_type=MESH)
        return (vir >= d).astype(jnp.int32) + (vir + d < nv).astype(jnp.int32)

    barrier = pltpu.get_barrier_semaphore()
    greeted = greet(barrier, ("occ", "aux")) + reach(barrier, 1)
    spans = [1 << i for i in range((nv - 1).bit_length())]
    rounds = [functools.partial(reach, d=d) for d in spans]
    rounds.append(functools.partial(greet, axes=("aux",)))
    owed = []

    def next_round():
        i = len(owed)
        if i:
            pl.semaphore_wait(enter.at[i - 1], owed[i - 1])
        if i < len(rounds):
            owed.append(rounds[i](enter.at[i]))
        elif i == len(rounds):
            owed.append(None)

    smalls = [
        pltpu.make_async_copy(*pair, small_sem.at[i])
        for i, pair in enumerate(
            ((rmask_hbm, right_mask), (pair_hbm, pair_mask), (lmask_hbm, left_mask), (res_hbm, res))
        )
    ]
    for copy in smalls[:2]:
        copy.start()
    raw_copy = pltpu.make_async_copy(right_hbm, raw, raw_sem)
    raw_copy.start()
    amp_copy = pltpu.make_async_copy(amp_hbm, amp, amp_sem)
    amp_copy.start()
    for copy in smalls[2:]:
        copy.start()

    def right_copy(u, m, down, big):
        block = rbuf.at[m, u] if big else rbuf.at[nq - 1, u, m - (nq - 1)]
        return pltpu.make_async_remote_copy(
            src_ref=block,
            dst_ref=block,
            send_sem=r_send.at[1 if down else 0, u, m],
            recv_sem=r_recv.at[u, m],
            device_id={"vir": vir - 1 if down else vir + 1},
            device_id_type=MESH,
        )

    def sized(m, act, ok=True):
        if isinstance(m, int):
            if 0 <= m < units:
                act(m < nq - 1)
            return

        @pl.when(ok & (m >= 0) & (m < nq - 1))
        def _():
            act(True)

        @pl.when(ok & (m >= nq - 1) & (m < units))
        def _():
            act(False)

    def send_own(m):
        def act(big):
            @pl.when(vir > 0)
            def _():
                right_copy(vir, m, True, big).start()

            @pl.when(vir < nv - 1)
            def _():
                right_copy(vir, m, False, big).start()

        sized(m, act)

    def arrive(k, m, forwarded, ok=True):
        def act(big):
            for down in (True, False):
                u = vir + k if down else vir - k
                here = u < nv if down else u >= 0
                passes = vir > 0 if down else vir < nv - 1

                @pl.when(here & (passes if forwarded else jnp.logical_not(passes)))
                def _():
                    right_copy(u, m, down, big).wait_recv()
                    if forwarded:
                        right_copy(u, m, down, big).start()

        sized(m, act, ok)

    def slot(m):
        for k in reversed(waves[:-1]):
            arrive(k, m - k + 1, True, (vir > 0) & (vir < nv - 1))
        if isinstance(m, int):
            if m == 0:
                send_own(AHEAD)
            elif m >= 2 * AHEAD:
                send_own(m + 1)
            elif m % 2:
                send_own(AHEAD + (m + 1) // 2)
        else:
            @pl.when((lax.rem(m, 2) == 1) & (m < 2 * AHEAD))
            def _():
                send_own(AHEAD + (m + 1) // 2)

            if units > 2 * AHEAD + 1:
                @pl.when(m >= 2 * AHEAD)
                def _():
                    send_own(m + 1)

    def left_copy(n):
        return pltpu.make_async_copy(
            left_hbm.at[:, :, pl.ds(pl.multiple_of(n * QC, QC), QC)],
            left.at[:, :, pl.ds(pl.multiple_of(n * QC, QC), QC)],
            left_sem.at[n],
        )

    sub_rows = min(rows, TILE)
    first = (occ * nv + vir) * rows

    def arrange(n, carry):
        for r in range(0, rows, sub_rows):
            m = right_mask[(first + r) // TILE, n * QC // TILE].astype(F32)
            x = raw[pl.ds(r, sub_rows), :, pl.ds(pl.multiple_of(n * QC, QC), QC)].astype(F32) * m
            for b in range(block_b):
                e = b % BB
                rbuf[n, vir, b // BB, r : r + sub_rows, e * QC : (e + 1) * QC] = x[:, b, :].astype(
                    BF16
                )
        return carry

    smalls[0].wait()
    raw_copy.wait()
    lax.fori_loop(0, nq, arrange, 0)
    smalls[1].wait()
    amp_copy.wait()
    for n in range(nq):
        left_copy(n).start()

    piece = min(cq, TILE)

    def masked(p, row, column):
        m = pair_mask[p, row // TILE, column // TILE].astype(F32)
        block = amp[
            p, pl.ds(pl.multiple_of(row, piece), piece), pl.ds(pl.multiple_of(column, TILE), TILE)
        ]
        return (block.astype(F32) * m).astype(BF16)

    def fill_send(p, carry):
        for k in range(1, no):
            base = lax.rem(occ + k, no) * depth
            for off in range(0, cq, piece):
                for col in range(0, depth, TILE):
                    tsend[k - 1, p, off : off + piece, col : col + TILE] = masked(
                        p, aux * cq + off, base + col
                    )
        return carry

    def occ_copy(k, h):
        return pltpu.make_async_remote_copy(
            src_ref=tsend.at[k - 1, pl.ds(h * pp, pp)],
            dst_ref=tau.at[occ, aux, pl.ds(h * pp, pp)],
            send_sem=t_send.at[k, 0, h],
            recv_sem=t_recv.at[occ, aux, h],
            device_id={"occ": lax.rem(occ + k, no)},
            device_id_type=MESH,
        )

    def aux_copy(k, sem, q, h, bit):
        side = lax.rem(occ + k, no)
        block = tau.at[side, q, pl.ds(h * pp, pp)]
        return pltpu.make_async_remote_copy(
            src_ref=block,
            dst_ref=block,
            send_sem=t_send.at[k, sem, h],
            recv_sem=t_recv.at[side, q, h],
            device_id={"aux": aux ^ bit},
            device_id_type=MESH,
        )

    lax.fori_loop(0, pairs, fill_send, 0)
    pl.semaphore_wait(barrier, greeted)
    for n in range(AHEAD):
        send_own(n)
    tau_sends = []
    for h in range(pieces):
        for k in range(1, no):
            copy = occ_copy(k, h)
            copy.start()
            tau_sends.append(copy)
    next_round()

    ba = block_b * block_a
    wide = block_b * block_a * 8
    src = lax.broadcasted_iota(jnp.int32, (wide, ba), 0) // 8
    dst = lax.broadcasted_iota(jnp.int32, (wide, ba), 1)
    pick[...] = (src == dst).astype(F32).astype(BF16)
    acc[...] = jnp.zeros_like(acc)
    lhs_b[...] = jnp.zeros_like(lhs_b)

    def fill_own(i, carry):
        p, q = i // na, lax.rem(i, na)
        for off in range(0, cq, piece):
            for col in range(0, depth, TILE):
                tau[occ, q, p, off : off + piece, col : col + TILE] = masked(
                    p, q * cq + off, occ * depth + col
                )
        return carry

    lax.fori_loop(0, pairs * na, fill_own, 0)

    bits = []
    bit = na // 2
    while bit:
        bits.append(bit)
        bit //= 2

    news = [[0]]
    have = [0]
    for bit in bits:
        news.append([m ^ bit for m in have])
        have = have + news[-1]
    sems = {}
    for s in range(len(news)):
        for m in news[s]:
            for later in range(s, len(bits)):
                sems[m, later] = len(sems) + 1

    def tau_stage(s, h):
        for k in range(1, no):
            for m in news[s]:
                q = aux ^ m
                aux_copy(k, 0, q, h, 0).wait_recv()
                for later in range(s, len(bits)):
                    copy = aux_copy(k, sems[m, later], q, h, bits[later])
                    copy.start()
                    tau_sends.append(copy)

    def prepare(i, carry):
        n, cs = i // steps, lax.rem(i, steps)

        @pl.when(cs == 0)
        def _():
            left_copy(n).wait()

        c0 = pl.multiple_of(cs * cc, cc)
        q0 = pl.multiple_of(n * QC, QC)
        lm = left_mask[cs * cc // TILE, n * QC // TILE].astype(F32)
        w = left[:, pl.ds(c0, cc), pl.ds(q0, QC)].astype(F32) * lm
        w = w.reshape(block_a, groups, 8, QC)
        for j in range(groups):
            rhs[i, :, j * QC : (j + 1) * QC] = w[:, j].reshape(block_a * 8, QC).astype(BF16)
        return carry

    smalls[2].wait()
    ready = 0
    done = 0
    for w in range(pieces + len(bits)):
        for s in range(len(news)):
            if 0 <= w - s < pieces:
                tau_stage(s, w - s)
        while done < lead and (done + 1) * (pieces + len(bits)) <= (w + 1) * lead:
            slot(done)
            done += 1
        if 0 < w <= len(rounds):
            next_round()
        upto = nq * steps * (w + 1) // (pieces + len(bits))
        lax.fori_loop(ready, upto, prepare, 0)
        ready = upto
    while done < lead:
        slot(done)
        done += 1
    while len(owed) <= len(rounds):
        next_round()
    lax.fori_loop(ready, nq * steps, prepare, 0)

    def stage_two(e, lhs, i):
        span = pl.ds(pl.multiple_of(e * (2 * BB * half), 2 * BB * half), 2 * BB * half)
        acc[span, :] += lax.dot_general(
            lhs[...], rhs[i], (((1,), (1,)), ((), ())), preferred_element_type=F32
        )

    def stage_one(n, e, cs, lhs):
        q, s = cs // subs, lax.rem(cs, subs)
        t = tau[:, q, :, pl.ds(pl.multiple_of(s * cc, cc), cc), :].reshape(pall * cc, depth)
        r = rbuf[n, :, e].reshape(depth, bq)
        inner = jnp.dot(t, r, preferred_element_type=F32)
        inner = inner.reshape(pall, groups, 8, bq)
        for j in range(groups):
            for e in range(BB):
                x = inner[:, j, :, e * QC : (e + 1) * QC].reshape(half, QC)
                hi = x.astype(BF16)
                lo = (x - hi.astype(F32)).astype(BF16)
                row = 2 * e * half
                lhs[row : row + half, j * QC : (j + 1) * QC] = hi
                lhs[row + half : row + 2 * half, j * QC : (j + 1) * QC] = lo

    def chunk(ch, carry):
        n, e = ch // nbp, lax.rem(ch, nbp)
        ending = n == nq - 1
        unit = jnp.where(ending, nq - 1 + e, n)

        @pl.when(ending | (e == 0))
        def _():
            for k in waves:
                arrive(k, unit, False)

        @pl.when((ending | (e == nbp - 1)) & (unit + lead < units + nv - 3))
        def _():
            slot(unit + lead)

        last = jnp.maximum(ch - 1, 0)
        for cs in range(steps):
            now, old = (lhs_a, lhs_b) if cs % 2 == 0 else (lhs_b, lhs_a)
            stage_one(n, e, cs, now)
            if cs == 0:
                stage_two(lax.rem(last, nbp), old, last // nbp * steps + steps - 1)
            else:
                stage_two(e, old, n * steps + cs - 1)
        return carry

    lax.fori_loop(0, nch, chunk, 0)
    stage_two(nbp - 1, lhs_b, nq * steps - 1)

    width = block_a * 8
    row_i = lax.rem(lax.broadcasted_iota(jnp.int32, (half, width), 0), 8)
    col_i = lax.rem(lax.broadcasted_iota(jnp.int32, (half, width), 1), 8)
    diag = (row_i == col_i).astype(F32)
    total = jnp.zeros((pall, ba), F32)
    for b in range(block_b):
        y = acc[2 * b * half : (2 * b + 1) * half, :] + acc[(2 * b + 1) * half : (2 * b + 2) * half, :]
        y = (y * diag).reshape(pall, 8, width).sum(axis=1)
        for _ in range(3):
            z = y.astype(BF16)
            total += jnp.dot(
                z, pick[b * width : (b + 1) * width, :], preferred_element_type=F32
            )
            y = y - z.astype(F32)
    part[...] = total.reshape(no, pairs, ba)

    devices = no * nv * na
    me = (occ * nv + vir) * na + aux
    parts[me] = part[occ]

    def final_copy(k):
        j = lax.rem(me + k, devices)
        to = (j // (nv * na), lax.rem(j // na, nv), lax.rem(j, na))
        return pltpu.make_async_remote_copy(
            src_ref=part.at[to[0]],
            dst_ref=parts.at[me],
            send_sem=a_send.at[k],
            recv_sem=a_recv.at[me],
            device_id=to,
            device_id_type=MESH,
        )

    def final_arrival(k):
        j = lax.rem(me + k, devices)
        to = (j // (nv * na), lax.rem(j // na, nv), lax.rem(j, na))
        return pltpu.make_async_remote_copy(
            src_ref=part.at[to[0]],
            dst_ref=parts.at[j],
            send_sem=a_send.at[k],
            recv_sem=a_recv.at[j],
            device_id=to,
            device_id_type=MESH,
        )

    def start_final(k, carry):
        final_copy(k).start()
        return carry

    def wait_final(k, carry):
        final_arrival(k).wait_recv()
        return carry

    def drain_final(k, carry):
        final_copy(k).wait_send()
        return carry

    lax.fori_loop(1, devices, start_final, 0)
    for copy in tau_sends:
        copy.wait_send()

    def drain_right(m, carry):
        def act(big):
            for down in (True, False):
                passes = vir > 0 if down else vir < nv - 1

                @pl.when(passes)
                def _():
                    right_copy(vir, m, down, big).wait_send()

                for k in waves:
                    u = vir + k if down else vir - k
                    here = u < nv if down else u >= 0

                    @pl.when(passes & here)
                    def _():
                        right_copy(u, m, down, big).wait_send()

        sized(m, act)
        return carry

    lax.fori_loop(0, units, drain_right, 0)
    lax.fori_loop(1, devices, wait_final, 0)
    smalls[3].wait()
    ladder = jnp.sum(parts[...], axis=0)
    for b in range(block_b):
        out[:, b, :] = res[:, b, :] + ladder[:, b * block_a : (b + 1) * block_a]
    lax.fori_loop(1, devices, drain_final, 0)


def local(sizes, amplitudes, pair_mask, left_factor, left_mask, right_factor, right_mask, residual_in):
    no, nv, na = sizes
    pairs, cols, virt = amplitudes.shape
    rows, block_b, auxn = right_factor.shape
    block_a = left_factor.shape[0]
    nq = auxn // QC
    units = nq - 1 + block_b // BB
    depth = rows * nv
    cq = cols // na
    pall = no * pairs
    ba = block_b * block_a
    vmem = pl.BlockSpec(memory_space=pltpu.VMEM)
    hbm = pl.BlockSpec(memory_space=pltpu.MemorySpace.HBM)
    dma = pltpu.SemaphoreType.DMA
    pieces = min(4, pairs)
    inner = min(CC, cq) // 8 * QC
    return pl.pallas_call(
        functools.partial(kernel, no, nv, na),
        out_shape=pltpu.VMEM(residual_in.shape, F32),
        in_specs=[hbm] * 7,
        out_specs=vmem,
        scratch_shapes=[
            pltpu.SMEM(pair_mask.shape, jnp.int32),
            pltpu.SMEM(left_mask.shape, jnp.int32),
            pltpu.SMEM(right_mask.shape, jnp.int32),
            pltpu.VMEM(residual_in.shape, F32),
            pltpu.VMEM((ba * 8, ba), BF16),
            pltpu.VMEM(right_factor.shape, BF16),
            pltpu.VMEM((pairs, cols, virt), BF16),
            pltpu.VMEM(left_factor.shape, BF16),
            pltpu.VMEM((nq, nv, block_b // BB, rows, BB * QC), BF16),
            pltpu.VMEM((no, na, pairs, cq, depth), BF16),
            pltpu.VMEM((max(no - 1, 1), pairs, cq, depth), BF16),
            pltpu.VMEM((nq * cols // min(CC, cq), block_a * 8, inner), BF16),
            pltpu.VMEM((2 * BB * pall * 8, inner), BF16),
            pltpu.VMEM((2 * BB * pall * 8, inner), BF16),
            pltpu.VMEM((2 * block_b * pall * 8, block_a * 8), F32),
            pltpu.VMEM((no, pairs, ba), F32),
            pltpu.VMEM((no * nv * na, pairs, ba), F32),
            dma((4,)),
            dma,
            dma((nq,)),
            dma,
            dma((2, nv, units)),
            dma((nv, units)),
            dma((no, 2 * na, pieces)),
            dma((no, na, pieces)),
            dma((no * nv * na,)),
            dma((no * nv * na,)),
            pltpu.SemaphoreType.REGULAR((nv.bit_length() + 1,)),
        ],
        compiler_params=pltpu.CompilerParams(
            collective_id=0, has_side_effects=True, vmem_limit_bytes=62 * 1024 * 1024
        ),
        name="ladder",
    )(pair_mask, left_mask, right_mask, amplitudes, left_factor, right_factor, residual_in)


def solution(mesh):
    sizes = tuple(mesh.shape[name] for name in ("occ", "vir", "aux"))
    return jax.shard_map(
        functools.partial(local, sizes),
        mesh=mesh,
        in_specs=(
            P("occ", "vir", None),
            P("occ", "vir", None),
            P(None, "vir", "aux"),
            P("vir", "aux"),
            P(("occ", "vir"), None, "aux"),
            P(None, "aux"),
            P("occ", None, None),
        ),
        out_specs=P("occ", None, None),
        check_vma=False,
    )
```

```python
import functools

import jax
import jax.numpy as jnp
from jax import lax
from jax.experimental import pallas as pl
from jax.experimental.pallas import tpu as pltpu
from jax.sharding import PartitionSpec as P

TILE = 128
QC = 128
CC = 64
BB = 2
AHEAD = 4
MESH = pl.DeviceIdType.MESH
F32 = jnp.float32
BF16 = jnp.bfloat16


def kernel(
    no, nv, na, pair_hbm, lmask_hbm, rmask_hbm, amp_hbm, left_hbm, right_hbm, res_hbm,
    out, pair_mask, left_mask, right_mask, res, pick, raw, amp, left, rbuf, tau, tsend, rhs, lhs_a, lhs_b, acc, part, parts,
    small_sem, amp_sem, left_sem, raw_sem, r_send, r_recv, t_send, t_recv, a_send, a_recv, enter,
):
    occ, vir, aux = lax.axis_index("occ"), lax.axis_index("vir"), lax.axis_index("aux")
    pairs, cols, virt = amp.shape
    nq, _, nbp, rows, bq = rbuf.shape
    block_b = raw.shape[1]
    nch = nq * nbp
    units = nq - 1 + nbp
    block_a = left.shape[0]
    cq, depth = tau.shape[3], tau.shape[4]
    pall = no * pairs
    cc = min(CC, cq)
    steps = cols // cc
    subs = cq // cc
    groups = cc // 8
    half = pall * 8
    pieces = min(4, pairs)
    pp = pairs // pieces
    waves = list(range(1, nv))
    lead = max(3, nv - 2)

    place = {"occ": (occ, no), "vir": (vir, nv), "aux": (aux, na)}

    def greet(sem, axes):
        count = 0
        for axis in axes:
            at, size = place[axis]
            for k in range(1, size):
                pl.semaphore_signal(
                    sem, inc=1, device_id={axis: lax.rem(at + k, size)}, device_id_type=MESH
                )
                count += 1
        return count

    def reach(sem, d):
        for ok, to in ((vir >= d, vir - d), (vir + d < nv, vir + d)):
            @pl.when(ok)
            def _():
                pl.semaphore_signal(sem, inc=1, device_id={"vir": to}, device_id_type=MESH)
        return (vir >= d).astype(jnp.int32) + (vir + d < nv).astype(jnp.int32)

    barrier = pltpu.get_barrier_semaphore()
    greeted = greet(barrier, ("occ", "aux")) + reach(barrier, 1)
    spans = [1 << i for i in range((nv - 1).bit_length())]
    rounds = [functools.partial(reach, d=d) for d in spans]
    rounds.append(functools.partial(greet, axes=("aux",)))
    owed = []

    def next_round():
        i = len(owed)
        if i:
            pl.semaphore_wait(enter.at[i - 1], owed[i - 1])
        if i < len(rounds):
            owed.append(rounds[i](enter.at[i]))
        elif i == len(rounds):
            owed.append(None)

    smalls = [
        pltpu.make_async_copy(*pair, small_sem.at[i])
        for i, pair in enumerate(
            ((rmask_hbm, right_mask), (pair_hbm, pair_mask), (lmask_hbm, left_mask), (res_hbm, res))
        )
    ]
    for copy in smalls[:2]:
        copy.start()
    raw_copy = pltpu.make_async_copy(right_hbm, raw, raw_sem)
    raw_copy.start()
    amp_copy = pltpu.make_async_copy(amp_hbm, amp, amp_sem)
    amp_copy.start()
    for copy in smalls[2:]:
        copy.start()

    def right_copy(u, m, down, big):
        block = rbuf.at[m, u] if big else rbuf.at[nq - 1, u, m - (nq - 1)]
        return pltpu.make_async_remote_copy(
            src_ref=block,
            dst_ref=block,
            send_sem=r_send.at[1 if down else 0, u, m],
            recv_sem=r_recv.at[u, m],
            device_id={"vir": vir - 1 if down else vir + 1},
            device_id_type=MESH,
        )

    def sized(m, act, ok=True):
        if isinstance(m, int):
            if 0 <= m < units:
                act(m < nq - 1)
            return

        @pl.when(ok & (m >= 0) & (m < nq - 1))
        def _():
            act(True)

        @pl.when(ok & (m >= nq - 1) & (m < units))
        def _():
            act(False)

    def send_own(m):
        def act(big):
            @pl.when(vir > 0)
            def _():
                right_copy(vir, m, True, big).start()

            @pl.when(vir < nv - 1)
            def _():
                right_copy(vir, m, False, big).start()

        sized(m, act)

    def arrive(k, m, forwarded, ok=True):
        def act(big):
            for down in (True, False):
                u = vir + k if down else vir - k
                here = u < nv if down else u >= 0
                passes = vir > 0 if down else vir < nv - 1

                @pl.when(here & (passes if forwarded else jnp.logical_not(passes)))
                def _():
                    right_copy(u, m, down, big).wait_recv()
                    if forwarded:
                        right_copy(u, m, down, big).start()

        sized(m, act, ok)

    def slot(m):
        for k in reversed(waves[:-1]):
            arrive(k, m - k + 1, True, (vir > 0) & (vir < nv - 1))
        if isinstance(m, int):
            if m == 0:
                send_own(AHEAD)
            elif m >= 2 * AHEAD:
                send_own(m + 1)
            elif m % 2:
                send_own(AHEAD + (m + 1) // 2)
        else:
            @pl.when((lax.rem(m, 2) == 1) & (m < 2 * AHEAD))
            def _():
                send_own(AHEAD + (m + 1) // 2)

            if units > 2 * AHEAD + 1:
                @pl.when(m >= 2 * AHEAD)
                def _():
                    send_own(m + 1)

    def left_copy(n):
        return pltpu.make_async_copy(
            left_hbm.at[:, :, pl.ds(pl.multiple_of(n * QC, QC), QC)],
            left.at[:, :, pl.ds(pl.multiple_of(n * QC, QC), QC)],
            left_sem.at[n],
        )

    sub_rows = min(rows, TILE)
    first = (occ * nv + vir) * rows

    def arrange(n, carry):
        for r in range(0, rows, sub_rows):
            m = right_mask[(first + r) // TILE, n * QC // TILE].astype(F32)
            x = raw[pl.ds(r, sub_rows), :, pl.ds(pl.multiple_of(n * QC, QC), QC)].astype(F32) * m
            for b in range(block_b):
                e = b % BB
                rbuf[n, vir, b // BB, r : r + sub_rows, e * QC : (e + 1) * QC] = x[:, b, :].astype(
                    BF16
                )
        return carry

    smalls[0].wait()
    raw_copy.wait()
    lax.fori_loop(0, nq, arrange, 0)
    smalls[1].wait()
    amp_copy.wait()
    for n in range(nq):
        left_copy(n).start()

    piece = min(cq, TILE)

    def masked(p, row, column):
        m = pair_mask[p, row // TILE, column // TILE].astype(F32)
        block = amp[
            p, pl.ds(pl.multiple_of(row, piece), piece), pl.ds(pl.multiple_of(column, TILE), TILE)
        ]
        return (block.astype(F32) * m).astype(BF16)

    def fill_send(p, carry):
        for k in range(1, no):
            base = lax.rem(occ + k, no) * depth
            for off in range(0, cq, piece):
                for col in range(0, depth, TILE):
                    tsend[k - 1, p, off : off + piece, col : col + TILE] = masked(
                        p, aux * cq + off, base + col
                    )
        return carry

    def occ_copy(k, h):
        return pltpu.make_async_remote_copy(
            src_ref=tsend.at[k - 1, pl.ds(h * pp, pp)],
            dst_ref=tau.at[occ, aux, pl.ds(h * pp, pp)],
            send_sem=t_send.at[k, 0, h],
            recv_sem=t_recv.at[occ, aux, h],
            device_id={"occ": lax.rem(occ + k, no)},
            device_id_type=MESH,
        )

    def aux_copy(k, sem, q, h, bit):
        side = lax.rem(occ + k, no)
        block = tau.at[side, q, pl.ds(h * pp, pp)]
        return pltpu.make_async_remote_copy(
            src_ref=block,
            dst_ref=block,
            send_sem=t_send.at[k, sem, h],
            recv_sem=t_recv.at[side, q, h],
            device_id={"aux": aux ^ bit},
            device_id_type=MESH,
        )

    lax.fori_loop(0, pairs, fill_send, 0)
    pl.semaphore_wait(barrier, greeted)
    for n in range(AHEAD):
        send_own(n)
    tau_sends = []
    for h in range(pieces):
        for k in range(1, no):
            copy = occ_copy(k, h)
            copy.start()
            tau_sends.append(copy)
    next_round()

    ba = block_b * block_a
    wide = block_b * block_a * 8
    src = lax.broadcasted_iota(jnp.int32, (wide, ba), 0) // 8
    dst = lax.broadcasted_iota(jnp.int32, (wide, ba), 1)
    pick[...] = (src == dst).astype(F32).astype(BF16)
    acc[...] = jnp.zeros_like(acc)
    lhs_b[...] = jnp.zeros_like(lhs_b)

    def fill_own(i, carry):
        p, q = i // na, lax.rem(i, na)
        for off in range(0, cq, piece):
            for col in range(0, depth, TILE):
                tau[occ, q, p, off : off + piece, col : col + TILE] = masked(
                    p, q * cq + off, occ * depth + col
                )
        return carry

    lax.fori_loop(0, pairs * na, fill_own, 0)

    bits = []
    bit = na // 2
    while bit:
        bits.append(bit)
        bit //= 2

    news = [[0]]
    have = [0]
    for bit in bits:
        news.append([m ^ bit for m in have])
        have = have + news[-1]
    sems = {}
    for s in range(len(news)):
        for m in news[s]:
            for later in range(s, len(bits)):
                sems[m, later] = len(sems) + 1

    def tau_stage(s, h):
        for k in range(1, no):
            for m in news[s]:
                q = aux ^ m
                aux_copy(k, 0, q, h, 0).wait_recv()
                for later in range(s, len(bits)):
                    copy = aux_copy(k, sems[m, later], q, h, bits[later])
                    copy.start()
                    tau_sends.append(copy)

    def prepare(i, carry):
        n, cs = i // steps, lax.rem(i, steps)

        @pl.when(cs == 0)
        def _():
            left_copy(n).wait()

        c0 = pl.multiple_of(cs * cc, cc)
        q0 = pl.multiple_of(n * QC, QC)
        lm = left_mask[cs * cc // TILE, n * QC // TILE].astype(F32)
        w = left[:, pl.ds(c0, cc), pl.ds(q0, QC)].astype(F32) * lm
        w = w.reshape(block_a, groups, 8, QC)
        for j in range(groups):
            rhs[i, :, j * QC : (j + 1) * QC] = w[:, j].reshape(block_a * 8, QC).astype(BF16)
        return carry

    smalls[2].wait()
    ready = 0
    done = 0
    for w in range(pieces + len(bits)):
        for s in range(len(news)):
            if 0 <= w - s < pieces:
                tau_stage(s, w - s)
        while done < lead and (done + 1) * (pieces + len(bits)) <= (w + 1) * lead:
            slot(done)
            done += 1
        if 0 < w <= len(rounds):
            next_round()
        upto = nq * steps * (w + 1) // (pieces + len(bits))
        lax.fori_loop(ready, upto, prepare, 0)
        ready = upto
    while done < lead:
        slot(done)
        done += 1
    while len(owed) <= len(rounds):
        next_round()
    lax.fori_loop(ready, nq * steps, prepare, 0)

    def stage_two(e, lhs, i):
        span = pl.ds(pl.multiple_of(e * (2 * BB * half), 2 * BB * half), 2 * BB * half)
        acc[span, :] += lax.dot_general(
            lhs[...], rhs[i], (((1,), (1,)), ((), ())), preferred_element_type=F32
        )

    def stage_one(n, e, cs, lhs):
        q, s = cs // subs, lax.rem(cs, subs)
        t = tau[:, q, :, pl.ds(pl.multiple_of(s * cc, cc), cc), :].reshape(pall * cc, depth)
        r = rbuf[n, :, e].reshape(depth, bq)
        inner = jnp.dot(t, r, preferred_element_type=F32)
        inner = inner.reshape(pall, groups, 8, bq)
        for j in range(groups):
            for e in range(BB):
                x = inner[:, j, :, e * QC : (e + 1) * QC].reshape(half, QC)
                hi = x.astype(BF16)
                lo = (x - hi.astype(F32)).astype(BF16)
                row = 2 * e * half
                lhs[row : row + half, j * QC : (j + 1) * QC] = hi
                lhs[row + half : row + 2 * half, j * QC : (j + 1) * QC] = lo

    def chunk(ch, carry):
        n, e = ch // nbp, lax.rem(ch, nbp)
        ending = n == nq - 1
        unit = jnp.where(ending, nq - 1 + e, n)

        @pl.when(ending | (e == 0))
        def _():
            for k in waves:
                arrive(k, unit, False)

        @pl.when((ending | (e == nbp - 1)) & (unit + lead < units + nv - 3))
        def _():
            slot(unit + lead)

        last = jnp.maximum(ch - 1, 0)
        for cs in range(steps):
            now, old = (lhs_a, lhs_b) if cs % 2 == 0 else (lhs_b, lhs_a)
            stage_one(n, e, cs, now)
            if cs == 0:
                stage_two(lax.rem(last, nbp), old, last // nbp * steps + steps - 1)
            else:
                stage_two(e, old, n * steps + cs - 1)
        return carry

    lax.fori_loop(0, nch, chunk, 0)
    stage_two(nbp - 1, lhs_b, nq * steps - 1)

    width = block_a * 8
    row_i = lax.rem(lax.broadcasted_iota(jnp.int32, (half, width), 0), 8)
    col_i = lax.rem(lax.broadcasted_iota(jnp.int32, (half, width), 1), 8)
    diag = (row_i == col_i).astype(F32)
    total = jnp.zeros((pall, ba), F32)
    for b in range(block_b):
        y = acc[2 * b * half : (2 * b + 1) * half, :] + acc[(2 * b + 1) * half : (2 * b + 2) * half, :]
        y = (y * diag).reshape(pall, 8, width).sum(axis=1)
        for _ in range(3):
            z = y.astype(BF16)
            total += jnp.dot(
                z, pick[b * width : (b + 1) * width, :], preferred_element_type=F32
            )
            y = y - z.astype(F32)
    part[...] = total.reshape(no, pairs, ba)

    devices = no * nv * na
    me = (occ * nv + vir) * na + aux
    parts[me] = part[occ]

    def final_copy(k):
        j = lax.rem(me + k, devices)
        to = (j // (nv * na), lax.rem(j // na, nv), lax.rem(j, na))
        return pltpu.make_async_remote_copy(
            src_ref=part.at[to[0]],
            dst_ref=parts.at[me],
            send_sem=a_send.at[k],
            recv_sem=a_recv.at[me],
            device_id=to,
            device_id_type=MESH,
        )

    def final_arrival(k):
        j = lax.rem(me + k, devices)
        to = (j // (nv * na), lax.rem(j // na, nv), lax.rem(j, na))
        return pltpu.make_async_remote_copy(
            src_ref=part.at[to[0]],
            dst_ref=parts.at[j],
            send_sem=a_send.at[k],
            recv_sem=a_recv.at[j],
            device_id=to,
            device_id_type=MESH,
        )

    def start_final(k, carry):
        final_copy(k).start()
        return carry

    def wait_final(k, carry):
        final_arrival(k).wait_recv()
        return carry

    def drain_final(k, carry):
        final_copy(k).wait_send()
        return carry

    lax.fori_loop(1, devices, start_final, 0)
    for copy in tau_sends:
        copy.wait_send()

    def drain_right(m, carry):
        def act(big):
            for down in (True, False):
                passes = vir > 0 if down else vir < nv - 1

                @pl.when(passes)
                def _():
                    right_copy(vir, m, down, big).wait_send()

                for k in waves:
                    u = vir + k if down else vir - k
                    here = u < nv if down else u >= 0

                    @pl.when(passes & here)
                    def _():
                        right_copy(u, m, down, big).wait_send()

        sized(m, act)
        return carry

    lax.fori_loop(0, units, drain_right, 0)
    lax.fori_loop(1, devices, drain_final, 0)
    lax.fori_loop(1, devices, wait_final, 0)
    smalls[3].wait()
    ladder = jnp.sum(parts[...], axis=0)
    for b in range(block_b):
        out[:, b, :] = res[:, b, :] + ladder[:, b * block_a : (b + 1) * block_a]


def local(sizes, amplitudes, pair_mask, left_factor, left_mask, right_factor, right_mask, residual_in):
    no, nv, na = sizes
    pairs, cols, virt = amplitudes.shape
    rows, block_b, auxn = right_factor.shape
    block_a = left_factor.shape[0]
    nq = auxn // QC
    units = nq - 1 + block_b // BB
    depth = rows * nv
    cq = cols // na
    pall = no * pairs
    ba = block_b * block_a
    vmem = pl.BlockSpec(memory_space=pltpu.VMEM)
    hbm = pl.BlockSpec(memory_space=pltpu.MemorySpace.HBM)
    dma = pltpu.SemaphoreType.DMA
    pieces = min(4, pairs)
    inner = min(CC, cq) // 8 * QC
    return pl.pallas_call(
        functools.partial(kernel, no, nv, na),
        out_shape=pltpu.VMEM(residual_in.shape, F32),
        in_specs=[hbm] * 7,
        out_specs=vmem,
        scratch_shapes=[
            pltpu.SMEM(pair_mask.shape, jnp.int32),
            pltpu.SMEM(left_mask.shape, jnp.int32),
            pltpu.SMEM(right_mask.shape, jnp.int32),
            pltpu.VMEM(residual_in.shape, F32),
            pltpu.VMEM((ba * 8, ba), BF16),
            pltpu.VMEM(right_factor.shape, BF16),
            pltpu.VMEM((pairs, cols, virt), BF16),
            pltpu.VMEM(left_factor.shape, BF16),
            pltpu.VMEM((nq, nv, block_b // BB, rows, BB * QC), BF16),
            pltpu.VMEM((no, na, pairs, cq, depth), BF16),
            pltpu.VMEM((max(no - 1, 1), pairs, cq, depth), BF16),
            pltpu.VMEM((nq * cols // min(CC, cq), block_a * 8, inner), BF16),
            pltpu.VMEM((2 * BB * pall * 8, inner), BF16),
            pltpu.VMEM((2 * BB * pall * 8, inner), BF16),
            pltpu.VMEM((2 * block_b * pall * 8, block_a * 8), F32),
            pltpu.VMEM((no, pairs, ba), F32),
            pltpu.VMEM((no * nv * na, pairs, ba), F32),
            dma((4,)),
            dma,
            dma((nq,)),
            dma,
            dma((2, nv, units)),
            dma((nv, units)),
            dma((no, 2 * na, pieces)),
            dma((no, na, pieces)),
            dma((no * nv * na,)),
            dma((no * nv * na,)),
            pltpu.SemaphoreType.REGULAR((nv.bit_length() + 1,)),
        ],
        compiler_params=pltpu.CompilerParams(
            collective_id=0, has_side_effects=True, vmem_limit_bytes=62 * 1024 * 1024
        ),
        name="ladder",
    )(pair_mask, left_mask, right_mask, amplitudes, left_factor, right_factor, residual_in)


def solution(mesh):
    sizes = tuple(mesh.shape[name] for name in ("occ", "vir", "aux"))
    return jax.shard_map(
        functools.partial(local, sizes),
        mesh=mesh,
        in_specs=(
            P("occ", "vir", None),
            P("occ", "vir", None),
            P(None, "vir", "aux"),
            P("vir", "aux"),
            P(("occ", "vir"), None, "aux"),
            P(None, "aux"),
            P("occ", None, None),
        ),
        out_specs=P("occ", None, None),
        check_vma=False,
    )
```
